256 devices in a mesh: group: 8 (over y, core), shard: 32 (over x, z).
Axes of the slice: x: 4, y: 4, z: 8, core: 2. Of those that a mesh axis runs over, the one named last changes fastest.
Arguments:
- params: float32 [4096, 7168], P(('group', 'shard')), may hold values from -3 to 3
- gradient: bfloat16 [4096, 7168], P(('group', 'shard'))
- first_moment: float32 [4096, 7168], P(('group', 'shard')), may hold values from -2 to 2
- second_moment: float32 [4096, 7168], P(('group', 'shard')), may hold values from 0.01 to 1
Outputs:
- new_params: float32 [4096, 7168], P(('group', 'shard'))
- new_first: float32 [4096, 7168], P(('group', 'shard'))
- new_second: float32 [4096, 7168], P(('group', 'shard'))
- replica: bfloat16 [4096, 7168], P('group')
The draws below stay inside these ranges and needn't reach their ends.
All inputs are finite; a program needn't handle non-finite values.
Results may differ from the reference program's by a relative error of at most 0.00055.
Values may be sent and summed in bfloat16 or wider, within the bound.
A program may use at most 64 MiB of HBM per device.

```python
import math
import jax
import jax.numpy as jnp

D = 7168
ROWS = 4096


def draw_gradient(key, part):
    key_noise, key_rows, key_cols = jax.random.split(key, 3)
    row_index = jnp.arange(ROWS, dtype=jnp.float32)
    row_ramp = 1.0 + 2.0 * row_index / max(ROWS - 1, 1)
    row_rough = jnp.exp(jax.random.uniform(key_rows, (ROWS,), jnp.float32, 0.0, math.log(10.0)))
    col_rough = jnp.exp(jax.random.uniform(key_cols, (D,), jnp.float32, 0.0, math.log(10.0)))
    base_noise = jax.random.normal(key_noise, (ROWS, D), jnp.float32)
    values = 0.1 * base_noise * (row_ramp * row_rough)[:, None] * col_rough[None, :]
    return values.astype(jnp.bfloat16)


def level_of(own_key, dims, shards, smallest, largest):
    def one(position, blocks):
        heights = jax.random.uniform(jax.random.fold_in(jax.random.fold_in(own_key, 6), position), (blocks,), jnp.float32, smallest / len(shards), largest / len(shards))
        return jnp.repeat(jnp.exp(heights), dims[position] // blocks).reshape((-1,) + (1,) * (len(dims) - position - 1))

    factor_of = one(*shards[0])
    for cut in shards[1:]:
        factor_of = factor_of * one(*cut)
    return factor_of


def scatter_about(rng, dims, spread, reach, cuts=(), kind=jnp.bfloat16):
    result = jax.random.normal(rng, dims, jnp.float32) * spread
    if len(cuts) > 0:
        result = level_of(rng, dims, cuts, -0.22, 0.18) * result
    return jnp.clip(result, min=-reach, max=reach).astype(kind)


def setup_inputs(seed: int = 0) -> dict:
    keys = jax.random.split(jax.random.key(seed), 5)
    params = scatter_about(keys[0], (ROWS, D), 0.5, 3.0, ((0, 256),), jnp.float32)
    gradient = draw_gradient(jax.random.fold_in(keys[4], 71), 0)
    first_moment = scatter_about(keys[2], (ROWS, D), 0.3, 2.0, ((0, 256),), jnp.float32)
    second_moment = jnp.clip(jnp.exp(math.log(1.0) - 4.6051702 * jax.random.uniform(keys[3], (ROWS, D), jnp.float32) ** level_of(keys[3], (ROWS, D), ((0, 256),), -0.2, 0.2)), 0.01, 1.0)
    return {"params": params, "gradient": gradient, "first_moment": first_moment, "second_moment": second_moment}


def reference(params, gradient, first_moment, second_moment):
    grad_full = gradient.astype(jnp.float32)
    norm_total = jnp.sum(grad_full * grad_full)
    clip_scale = jnp.minimum(jnp.float32(1.0), 1.0 / jnp.sqrt(norm_total / (ROWS * D) + 1e-06))
    clipped = clip_scale * grad_full
    new_first = 0.9 * first_moment + 0.1 * clipped
    new_second = 0.95 * second_moment + 0.05 * clipped * clipped
    correct_one = 1.0 - 0.9 ** 10
    correct_two = 1.0 - 0.95 ** 10
    advance = new_first / correct_one / (jnp.sqrt(new_second / correct_two) + 1e-08)
    new_params = params - 0.1 * (advance + 0.1 * params)
    return (new_params, new_first, new_second, new_params.astype(jnp.bfloat16))
```

```python
import functools
import heapq
import itertools

import jax
import jax.numpy as jnp
from jax import lax
from jax.experimental import pallas as pl
from jax.experimental.pallas import tpu as pltpu
from jax.sharding import PartitionSpec as P

MESH = pl.DeviceIdType.MESH
NG, NX, NZ = 8, 4, 8
LANES = 128
ROWS = 8


def pieces_of(width):
    cut = (width // LANES * 23 // 56) * LANES
    return (
        (0, cut, width - cut, False, 1, 1),
        (8, cut, width - cut, False, -1, -1),
        (0, 0, cut, True, 1, 1),
        (8, 0, cut, True, -1, -1),
    )


def trees_of(pieces):
    sends = {}
    for v, (_, _, _, x_first, sx, sz) in enumerate(pieces):
        reach = {
            "x": {sx: NX // 2, -sx: NX // 2 - 1},
            "z": {sz: NZ // 2, -sz: NZ // 2 - 1},
        }
        first, second = ("x", "z") if x_first else ("z", "x")

        def add(axis, step, a, b, a2, b2):
            here = (a, b) if x_first else (b, a)
            there = (a2, b2) if x_first else (b2, a2)
            sends.setdefault((v, *here), []).append((axis, step, (v, *there)))

        for a in range(-reach[first][-1], reach[first][1] + 1):
            for step in (1, -1):
                if a * step >= 0 and abs(a) < reach[first][step]:
                    add(first, step, a, 0, a + step, 0)
            for step in (1, -1):
                for b in range(reach[second][step]):
                    add(second, step, a, b * step, a, (b + 1) * step)
    return sends


def order_of(pieces, sends, rate=46.6e3, latency=1.5):
    queues = {link: [] for link in itertools.product("xz", (1, -1))}
    free = dict.fromkeys(queues, 0.0)
    count = itertools.count()
    events = [(0.02 * v, next(count), (v, 0, 0)) for v in range(len(pieces))]
    events += [(0.0, next(count), None)]
    heapq.heapify(events)
    order = []
    while events:
        now, _, place = heapq.heappop(events)
        if place is not None:
            order.append(place)
            for axis, step, there in sends.get(place, ()):
                queues[axis, step].append(there)
        for link, queue in queues.items():
            if queue and free[link] <= now + 1e-9:
                there = queue.pop(0)
                free[link] = now + pieces[there[0]][2] * ROWS * 2 / rate
                heapq.heappush(events, (free[link], next(count), None))
                heapq.heappush(events, (free[link] + latency, next(count), there))
    return [place for place in order if place[1:] != (0, 0)]


def step_kernel(
    entries,
    p_hbm,
    g_hbm,
    m_hbm,
    v_hbm,
    rep,
    p_out,
    m_out,
    v_out,
    p_in,
    g_in,
    m_in,
    v_in,
    y_buf,
    x_buf,
    z_buf,
    load_sem,
    sum_send,
    sum_recv,
    send_sem,
    recv_sem,
):
    width = g_hbm.shape[1]
    group = lax.axis_index("group")
    shard = lax.axis_index("shard")
    x, z = shard // NZ, shard % NZ

    def at_group(k):
        return ((group + k) % NG, shard)

    def at(dx, dz):
        return (group, (x + dx + NX) % NX * NZ + (z + dz + NZ) % NZ)

    loads = [
        pltpu.make_async_copy(src, dst, load_sem.at[i])
        for i, (src, dst) in enumerate(
            ((g_hbm, g_in), (p_hbm, p_in), (m_hbm, m_in), (v_hbm, v_in))
        )
    ]
    for load in loads:
        load.start()

    stages = (
        (y_buf, [at_group(k) for k in range(1, NG)]),
        (x_buf, [at(k, 0) for k in range(1, NX)]),
        (z_buf, [at(0, k) for k in range(1, NZ)]),
    )
    barrier = pltpu.get_barrier_semaphore()
    peers = [peer for _, those in stages for peer in those]
    for peer in peers:
        pl.semaphore_signal(barrier, inc=1, device_id=peer, device_id_type=MESH)

    loads[0].wait()
    total = jnp.zeros((16, LANES), jnp.float32)
    for c in range(0, width, LANES):
        part = g_in[:, c : c + LANES].astype(jnp.float32)
        total = total + part * part
    total = jnp.sum(total, axis=0, keepdims=True)

    pl.semaphore_wait(barrier, len(peers))
    sent = []
    base = 0
    for buf, those in stages:
        buf[0] = total
        copies = [
            pltpu.make_async_remote_copy(
                src_ref=buf.at[0],
                dst_ref=buf.at[k],
                send_sem=sum_send.at[base + k - 1],
                recv_sem=sum_recv.at[base + k - 1],
                device_id=peer,
                device_id_type=MESH,
            )
            for k, peer in enumerate(those, 1)
        ]
        for copy in copies:
            copy.start()
        for copy in copies:
            copy.wait_recv()
        total = buf[0]
        for k in range(1, len(those) + 1):
            total = total + buf[k]
        sent += copies
        base += len(those)

    norm_total = jnp.sum(total, axis=1, keepdims=True)
    scale = jnp.minimum(1.0, 1.0 / jnp.sqrt(norm_total / entries + 1e-06))
    for load in loads[1:]:
        load.wait()

    pieces = pieces_of(width)
    sends = trees_of(pieces)
    order = order_of(pieces, sends)
    slot = {place: i for i, place in enumerate(order)}

    def view(place):
        v, ox, oz = place
        row, column, columns, *_ = pieces[v]
        source = (x - ox + NX) % NX * NZ + (z - oz + NZ) % NZ
        start = pl.multiple_of(source * 16 + row, 8)
        return rep.at[pl.ds(start, ROWS), pl.ds(column, columns)]

    def copy_to(axis, step, there):
        v, ox, oz = there
        here = (v, ox - step, oz) if axis == "x" else (v, ox, oz - step)
        return pltpu.make_async_remote_copy(
            src_ref=view(here),
            dst_ref=view(here),
            send_sem=send_sem.at[slot[there]],
            recv_sem=recv_sem.at[slot[there]],
            device_id=at(step, 0) if axis == "x" else at(0, step),
            device_id_type=MESH,
        )

    def forward(place):
        for axis, step, there in sends.get(place, ()):
            copy = copy_to(axis, step, there)
            copy.start()
            sent.append(copy)

    correct_one = 1.0 - 0.9**10
    correct_two = 1.0 - 0.95**10
    mine = pl.multiple_of(shard * 16, 16)
    chunk = 8 * LANES
    for v, (row, column, columns, *_) in enumerate(pieces):
        rows = slice(row, row + ROWS)
        for c in range(column, column + columns, chunk):
            cols = slice(c, min(c + chunk, column + columns))
            clipped = scale * g_in[rows, cols].astype(jnp.float32)
            params = p_in[rows, cols]
            new_first = 0.9 * m_in[rows, cols] + 0.1 * clipped
            new_second = 0.95 * v_in[rows, cols] + 0.05 * clipped * clipped
            stepped = (new_first / correct_one) / (
                jnp.sqrt(new_second / correct_two) + 1e-08
            )
            new_params = params - 0.1 * (stepped + 0.1 * params)
            p_out[rows, cols] = new_params
            m_out[rows, cols] = new_first
            v_out[rows, cols] = new_second
            rep[pl.ds(mine + row, ROWS), cols] = new_params.astype(jnp.bfloat16)
        forward((v, 0, 0))

    arrival = {
        there: (axis, step) for those in sends.values() for axis, step, there in those
    }
    for place in order:
        copy_to(*arrival[place], place).wait_recv()
        forward(place)
    for copy in sent:
        copy.wait_send()


def store_kernel(rep, p_new, m_new, v_new, p_out, m_out, v_out, rep_out, sem):
    parts = 8
    rows = rep.shape[0] // parts
    copies = [
        (rep.at[pl.ds(i * rows, rows)], rep_out.at[pl.ds(i * rows, rows)])
        for i in range(parts)
    ]
    copies += [(p_new, p_out), (m_new, m_out), (v_new, v_out)]
    started = [
        pltpu.make_async_copy(src, dst, sem.at[i]) for i, (src, dst) in enumerate(copies)
    ]
    for copy in started:
        copy.start()
    for copy in started:
        copy.wait()


def on_device(params, gradient, first_moment, second_moment):
    rows, width = params.shape
    entries = rows * width * lax.axis_size("group") * lax.axis_size("shard")
    whole = (rows * lax.axis_size("shard"), width)
    f32, bf16 = jnp.float32, jnp.bfloat16
    messages = 4 * (NX * NZ - 1)
    hbm = pl.BlockSpec(memory_space=pltpu.HBM)
    vmem = pl.BlockSpec(memory_space=pltpu.VMEM)
    rep, p_new, m_new, v_new = pl.pallas_call(
        functools.partial(step_kernel, entries),
        out_shape=(
            pltpu.VMEM(whole, bf16),
            pltpu.VMEM((rows, width), f32),
            pltpu.VMEM((rows, width), f32),
            pltpu.VMEM((rows, width), f32),
        ),
        in_specs=[hbm] * 4,
        out_specs=[vmem] * 4,
        scratch_shapes=[
            pltpu.VMEM((rows, width), f32),
            pltpu.VMEM((rows, width), bf16),
            pltpu.VMEM((rows, width), f32),
            pltpu.VMEM((rows, width), f32),
            pltpu.VMEM((NG, 1, LANES), f32),
            pltpu.VMEM((NX, 1, LANES), f32),
            pltpu.VMEM((NZ, 1, LANES), f32),
            pltpu.SemaphoreType.DMA((4,)),
            pltpu.SemaphoreType.DMA((NG + NX + NZ - 3,)),
            pltpu.SemaphoreType.DMA((NG + NX + NZ - 3,)),
            pltpu.SemaphoreType.DMA((messages,)),
            pltpu.SemaphoreType.DMA((messages,)),
        ],
        compiler_params=pltpu.CompilerParams(
            collective_id=0, has_side_effects=True, vmem_limit_bytes=58_200_000
        ),
        name="step",
    )(params, gradient, first_moment, second_moment)
    return pl.pallas_call(
        store_kernel,
        out_shape=(
            jax.ShapeDtypeStruct((rows, width), f32),
            jax.ShapeDtypeStruct((rows, width), f32),
            jax.ShapeDtypeStruct((rows, width), f32),
            jax.ShapeDtypeStruct(whole, bf16),
        ),
        in_specs=[vmem] * 4,
        out_specs=[hbm] * 4,
        scratch_shapes=[pltpu.SemaphoreType.DMA((11,))],
        compiler_params=pltpu.CompilerParams(vmem_limit_bytes=24 * 2**20),
        name="store",
    )(rep, p_new, m_new, v_new)


def solution(mesh):
    rows = P(("group", "shard"), None)
    return jax.shard_map(
        on_device,
        mesh=mesh,
        in_specs=(rows,) * 4,
        out_specs=(rows, rows, rows, P("group", None)),
        check_vma=False,
    )
```

```python
import functools
import heapq
import itertools

import jax
import jax.numpy as jnp
from jax import lax
from jax.experimental import pallas as pl
from jax.experimental.pallas import tpu as pltpu
from jax.sharding import PartitionSpec as P

MESH = pl.DeviceIdType.MESH
NG, NX, NZ = 8, 4, 8
LANES = 128
ROWS = 8


def pieces_of(width):
    cut = (width // LANES * 23 // 56) * LANES
    return (
        (0, cut, width - cut, False, 1, 1),
        (8, cut, width - cut, False, -1, -1),
        (0, 0, cut, True, 1, 1),
        (8, 0, cut, True, -1, -1),
    )


def trees_of(pieces):
    sends = {}
    for v, (_, _, _, x_first, sx, sz) in enumerate(pieces):
        reach = {
            "x": {sx: NX // 2, -sx: NX // 2 - 1},
            "z": {sz: NZ // 2, -sz: NZ // 2 - 1},
        }
        first, second = ("x", "z") if x_first else ("z", "x")

        def add(axis, step, a, b, a2, b2):
            here = (a, b) if x_first else (b, a)
            there = (a2, b2) if x_first else (b2, a2)
            sends.setdefault((v, *here), []).append((axis, step, (v, *there)))

        for a in range(-reach[first][-1], reach[first][1] + 1):
            for step in (1, -1):
                if a * step >= 0 and abs(a) < reach[first][step]:
                    add(first, step, a, 0, a + step, 0)
            for step in (1, -1):
                for b in range(reach[second][step]):
                    add(second, step, a, b * step, a, (b + 1) * step)
    return sends


def plan_of(pieces, sends, rate=46.6e3, latency=1.8, ahead=1.5):
    @functools.cache
    def depth(place):
        return max((1 + depth(there) for *_, there in sends.get(place, ())), default=0)

    queues = {link: [] for link in itertools.product("xz", (1, -1))}
    free = dict.fromkeys(queues, 0.0)
    count = itertools.count()
    events = [(0.15 * v, next(count), (v, 0, 0)) for v in range(len(pieces))]
    steps, held, turns = [], {}, []
    while events:
        now = events[0][0]
        while events and events[0][0] <= now + 1e-9:
            _, _, place = heapq.heappop(events)
            if place is not None:
                for axis, step, there in sends.get(place, ()):
                    heapq.heappush(
                        queues[axis, step], (-depth(there), next(count), there)
                    )
                    held[there] = len(steps)
                steps.append((now, place, []))
        for link, queue in queues.items():
            if queue and free[link] <= now + 1e-9:
                _, _, there = heapq.heappop(queue)
                free[link] = now + pieces[there[0]][2] * ROWS * 2 / rate
                heapq.heappush(events, (free[link], next(count), None))
                heapq.heappush(events, (free[link] + latency, next(count), there))
                turns.append((now, link, there))
    last = dict.fromkeys(queues, 0)
    for turn, link, there in turns:
        i = held[there]
        while i + 1 < len(steps) and steps[i + 1][0] <= turn - ahead:
            i += 1
        last[link] = max(i, last[link])
        steps[last[link]][2].append((*link, there))
    return [(place, starts) for _, place, starts in steps]


def step_kernel(
    entries,
    p_hbm,
    g_hbm,
    m_hbm,
    v_hbm,
    rep,
    p_out,
    m_out,
    v_out,
    p_in,
    g_in,
    m_in,
    v_in,
    plane_buf,
    z_buf,
    load_sem,
    sum_send,
    sum_recv,
    send_sem,
    recv_sem,
):
    width = g_hbm.shape[1]
    group = lax.axis_index("group")
    shard = lax.axis_index("shard")
    x, z = shard // NZ, shard % NZ

    def at(dx, dz, dg=0):
        to = (x + dx + NX) % NX * NZ + (z + dz + NZ) % NZ
        return ((group + dg) % NG, to)

    loads = [
        pltpu.make_async_copy(src, dst, load_sem.at[i])
        for i, (src, dst) in enumerate(
            ((g_hbm, g_in), (p_hbm, p_in), (m_hbm, m_in), (v_hbm, v_in))
        )
    ]
    for load in loads:
        load.start()

    stages = (
        (plane_buf, [at(k // NG, 0, k % NG) for k in range(1, NX * NG)]),
        (z_buf, [at(0, k) for k in range(1, NZ)]),
    )
    barrier = pltpu.get_barrier_semaphore()
    peers = [peer for _, those in stages for peer in those]
    for peer in reversed(peers):
        pl.semaphore_signal(barrier, inc=1, device_id=peer, device_id_type=MESH)

    loads[0].wait()
    total = jnp.zeros((16, LANES), jnp.float32)
    for c in range(0, width, LANES):
        part = g_in[:, c : c + LANES].astype(jnp.float32)
        total = total + part * part
    total = jnp.sum(total, axis=0, keepdims=True)

    pl.semaphore_wait(barrier, len(peers))
    summed = []
    for i, (buf, those) in enumerate(stages):
        buf[0] = total

        def message(src, dst, peer):
            return pltpu.make_async_remote_copy(
                src_ref=buf.at[src],
                dst_ref=buf.at[dst],
                send_sem=sum_send.at[i],
                recv_sem=sum_recv.at[i],
                device_id=peer,
                device_id_type=MESH,
            )

        for k, peer in enumerate(those, 1):
            message(0, k, peer).start()
        others = pl.ds(1, len(those))
        every = message(others, others, those[0])
        every.wait_recv()
        summed.append(every)
        total = jnp.sum(buf[...], axis=0)

    norm_total = jnp.sum(total, axis=1, keepdims=True)
    scale = jnp.minimum(1.0, 1.0 / jnp.sqrt(norm_total / entries + 1e-06))
    for load in loads[1:]:
        load.wait()

    pieces = pieces_of(width)
    sends = trees_of(pieces)
    plan = plan_of(pieces, sends)
    ends = [place for place, _ in plan if place not in sends]
    waits = [place for place, _ in plan[len(pieces) :] if place in sends]
    slot = {place: i for i, place in enumerate(waits)}
    sizes = sorted({piece[1:3] for piece in pieces})
    for place in ends:
        slot[place] = len(waits) + sizes.index(pieces[place[0]][1:3])

    def view(place):
        v, ox, oz = place
        row, column, columns, *_ = pieces[v]
        source = (x - ox + NX) % NX * NZ + (z - oz + NZ) % NZ
        start = pl.multiple_of(source * 16 + row, 8)
        return rep.at[pl.ds(start, ROWS), pl.ds(column, columns)]

    def copy_to(axis, step, there):
        v, ox, oz = there
        here = (v, ox - step, oz) if axis == "x" else (v, ox, oz - step)
        return pltpu.make_async_remote_copy(
            src_ref=view(here),
            dst_ref=view(here),
            send_sem=send_sem.at[0],
            recv_sem=recv_sem.at[slot[there]],
            device_id=at(step, 0) if axis == "x" else at(0, step),
            device_id_type=MESH,
        )

    def start(starts):
        for axis, step, there in starts:
            copy_to(axis, step, there).start()

    correct_one = 1.0 - 0.9**10
    correct_two = 1.0 - 0.95**10
    mine = pl.multiple_of(shard * 16, 16)
    chunk = 8 * LANES
    for v, (row, column, columns, *_) in enumerate(pieces):
        rows = slice(row, row + ROWS)
        for c in range(column, column + columns, chunk):
            cols = slice(c, min(c + chunk, column + columns))
            clipped = scale * g_in[rows, cols].astype(jnp.float32)
            params = p_in[rows, cols]
            new_first = 0.9 * m_in[rows, cols] + 0.1 * clipped
            new_second = 0.95 * v_in[rows, cols] + 0.05 * clipped * clipped
            stepped = (new_first / correct_one) / (
                jnp.sqrt(new_second / correct_two) + 1e-08
            )
            new_params = params - 0.1 * (stepped + 0.1 * params)
            p_out[rows, cols] = new_params
            m_out[rows, cols] = new_first
            v_out[rows, cols] = new_second
            rep[pl.ds(mine + row, ROWS), cols] = new_params.astype(jnp.bfloat16)
        start(plan[v][1])

    arrival = {
        there: (axis, step) for those in sends.values() for axis, step, there in those
    }
    for place, starts in plan[len(pieces) :]:
        if place in sends:
            copy_to(*arrival[place], place).wait_recv()
        start(starts)
    sent = rep.at[pl.ds(0, rep.shape[0] - 16)]
    pltpu.make_async_remote_copy(
        src_ref=sent,
        dst_ref=sent,
        send_sem=send_sem.at[0],
        recv_sem=recv_sem.at[0],
        device_id=at(1, 0),
        device_id_type=MESH,
    ).wait_send()
    for every in summed:
        every.wait_send()
    for i, (column, columns) in enumerate(sizes):
        these = [place for place in ends if pieces[place[0]][1] == column]
        taken = rep.at[pl.ds(0, len(these) * ROWS), pl.ds(column, columns)]
        pltpu.make_async_remote_copy(
            src_ref=taken,
            dst_ref=taken,
            send_sem=send_sem.at[0],
            recv_sem=recv_sem.at[len(waits) + i],
            device_id=at(1, 0),
            device_id_type=MESH,
        ).wait_recv()


def store_kernel(rep, p_new, m_new, v_new, p_out, m_out, v_out, rep_out, sem):
    parts = 8
    rows = rep.shape[0] // parts
    copies = [
        (rep.at[pl.ds(i * rows, rows)], rep_out.at[pl.ds(i * rows, rows)])
        for i in range(parts)
    ]
    copies += [(p_new, p_out), (m_new, m_out), (v_new, v_out)]
    started = [
        pltpu.make_async_copy(src, dst, sem.at[i]) for i, (src, dst) in enumerate(copies)
    ]
    for copy in started:
        copy.start()
    for copy in started:
        copy.wait()


def on_device(params, gradient, first_moment, second_moment):
    rows, width = params.shape
    entries = rows * width * lax.axis_size("group") * lax.axis_size("shard")
    whole = (rows * lax.axis_size("shard"), width)
    f32, bf16 = jnp.float32, jnp.bfloat16
    messages = 78
    hbm = pl.BlockSpec(memory_space=pltpu.HBM)
    vmem = pl.BlockSpec(memory_space=pltpu.VMEM)
    rep, p_new, m_new, v_new = pl.pallas_call(
        functools.partial(step_kernel, entries),
        out_shape=(
            pltpu.VMEM(whole, bf16),
            pltpu.VMEM((rows, width), f32),
            pltpu.VMEM((rows, width), f32),
            pltpu.VMEM((rows, width), f32),
        ),
        in_specs=[hbm] * 4,
        out_specs=[vmem] * 4,
        scratch_shapes=[
            pltpu.VMEM((rows, width), f32),
            pltpu.VMEM((rows, width), bf16),
            pltpu.VMEM((rows, width), f32),
            pltpu.VMEM((rows, width), f32),
            pltpu.VMEM((NX * NG, 1, LANES), f32),
            pltpu.VMEM((NZ, 1, LANES), f32),
            pltpu.SemaphoreType.DMA((4,)),
            pltpu.SemaphoreType.DMA((2,)),
            pltpu.SemaphoreType.DMA((2,)),
            pltpu.SemaphoreType.DMA((1,)),
            pltpu.SemaphoreType.DMA((messages,)),
        ],
        compiler_params=pltpu.CompilerParams(
            collective_id=0, has_side_effects=True, vmem_limit_bytes=58_200_000
        ),
        name="step",
    )(params, gradient, first_moment, second_moment)
    return pl.pallas_call(
        store_kernel,
        out_shape=(
            jax.ShapeDtypeStruct((rows, width), f32),
            jax.ShapeDtypeStruct((rows, width), f32),
            jax.ShapeDtypeStruct((rows, width), f32),
            jax.ShapeDtypeStruct(whole, bf16),
        ),
        in_specs=[vmem] * 4,
        out_specs=[hbm] * 4,
        scratch_shapes=[pltpu.SemaphoreType.DMA((11,))],
        compiler_params=pltpu.CompilerParams(vmem_limit_bytes=24 * 2**20),
        name="store",
    )(rep, p_new, m_new, v_new)


def solution(mesh):
    rows = P(("group", "shard"), None)
    return jax.shard_map(
        on_device,
        mesh=mesh,
        in_specs=(rows,) * 4,
        out_specs=(rows, rows, rows, P("group", None)),
        check_vma=False,
    )
```

```python
import functools
import heapq
import itertools

import jax
import jax.numpy as jnp
from jax import lax
from jax.experimental import pallas as pl
from jax.experimental.pallas import tpu as pltpu
from jax.sharding import PartitionSpec as P

MESH = pl.DeviceIdType.MESH
NY, NX, NZ = 4, 4, 8
LANES = 128
ROWS = 8


def pieces_of(width):
    cut = (width // LANES * 23 // 56) * LANES
    return (
        (0, cut, width - cut, False, 1, 1),
        (8, cut, width - cut, False, -1, -1),
        (0, 0, cut, True, 1, 1),
        (8, 0, cut, True, -1, -1),
    )


def trees_of(pieces):
    sends = {}
    for v, (_, _, _, x_first, sx, sz) in enumerate(pieces):
        reach = {
            "x": {sx: NX // 2, -sx: NX // 2 - 1},
            "z": {sz: NZ // 2, -sz: NZ // 2 - 1},
        }
        first, second = ("x", "z") if x_first else ("z", "x")

        def add(axis, step, a, b, a2, b2):
            here = (a, b) if x_first else (b, a)
            there = (a2, b2) if x_first else (b2, a2)
            sends.setdefault((v, *here), []).append((axis, step, (v, *there)))

        for a in range(-reach[first][-1], reach[first][1] + 1):
            for step in (1, -1):
                if a * step >= 0 and abs(a) < reach[first][step]:
                    add(first, step, a, 0, a + step, 0)
            for step in (1, -1):
                for b in range(reach[second][step]):
                    add(second, step, a, b * step, a, (b + 1) * step)
    return sends


def plan_of(pieces, sends, rate=46.6e3, latency=2.4, ahead=1.5):
    @functools.cache
    def depth(place):
        return max((1 + depth(there) for *_, there in sends.get(place, ())), default=0)

    queues = {link: [] for link in itertools.product("xz", (1, -1))}
    free = dict.fromkeys(queues, 0.0)
    count = itertools.count()
    events = [(0.15 * v, next(count), (v, 0, 0)) for v in range(len(pieces))]
    steps, held, turns = [], {}, []
    while events:
        now = events[0][0]
        while events and events[0][0] <= now + 1e-9:
            _, _, place = heapq.heappop(events)
            if place is not None:
                for axis, step, there in sends.get(place, ()):
                    heapq.heappush(
                        queues[axis, step], (-depth(there), next(count), there)
                    )
                    held[there] = len(steps)
                steps.append((now, place, []))
        for link, queue in queues.items():
            if queue and free[link] <= now + 1e-9:
                _, _, there = heapq.heappop(queue)
                free[link] = now + pieces[there[0]][2] * ROWS * 2 / rate
                heapq.heappush(events, (free[link], next(count), None))
                heapq.heappush(events, (free[link] + latency, next(count), there))
                turns.append((now, link, there))
    last = dict.fromkeys(queues, 0)
    for turn, link, there in turns:
        i = held[there]
        while i + 1 < len(steps) and steps[i + 1][0] <= turn - ahead:
            i += 1
        last[link] = max(i, last[link])
        steps[last[link]][2].append((*link, there))
    return [(place, starts) for _, place, starts in steps]


def source_of(send):
    axis, step, (v, ox, oz) = send
    return (v, ox - step, oz) if axis == "x" else (v, ox, oz - step)


def waits_of(pieces, sends, plan):
    there_by = {place: i for i, (place, _) in enumerate(plan)}
    needed = {}
    for i, (_, starts) in enumerate(plan):
        for send in starts:
            needed.setdefault(source_of(send), i)
    waits = [[] for _ in range(len(plan) + 1)]
    for size in sorted({piece[1:3] for piece in pieces}):
        left = sorted(
            (needed.get(place, len(plan)), i, place)
            for place, i in there_by.items()
            if i >= len(pieces) and pieces[place[0]][1:3] == size
        )
        while left:
            at = left[0][0]
            waits[at].append([place for _, i, place in left if i <= at])
            left = [entry for entry in left if entry[1] > at]
    return waits


def far_first(offsets):
    def chips(to):
        sizes = (NX, NZ, NY)
        return sum(min(step, size - step) for step, size in zip(to, sizes))

    return sorted(offsets, key=chips, reverse=True)


def step_kernel(
    entries,
    p_hbm,
    g_hbm,
    m_hbm,
    v_hbm,
    rep,
    p_out,
    m_out,
    v_out,
    p_in,
    g_in,
    m_in,
    v_in,
    own_buf,
    plane_buf,
    z_buf,
    all_buf,
    load_sem,
    sum_send,
    sum_recv,
    send_sem,
    recv_sem,
):
    width = g_hbm.shape[1]
    group = lax.axis_index("group")
    shard = lax.axis_index("shard")
    x, z = shard // NZ, shard % NZ

    y, core = group // 2, group % 2
    hub = core == 1

    def at(dx, dz, dy=0, to_core=core):
        to = (x + dx + NX) % NX * NZ + (z + dz + NZ) % NZ
        return ((y + dy + NY) % NY * 2 + to_core, to)

    loads = [
        pltpu.make_async_copy(src, dst, load_sem.at[i])
        for i, (src, dst) in enumerate(
            ((g_hbm, g_in), (p_hbm, p_in), (m_hbm, m_in), (v_hbm, v_in))
        )
    ]
    loads[0].start()

    plane = far_first((dx, 0, dy) for dx in range(NX) for dy in range(NY))
    line = far_first((0, dz, 0) for dz in range(NZ))
    near = ((1, 0), (-1, 0), (0, 1), (0, -1))
    barrier = pltpu.get_barrier_semaphore()

    def greet(peer):
        pl.semaphore_signal(barrier, inc=1, device_id=peer, device_id_type=MESH)

    @pl.when(hub)
    def _():
        for to in (*line[:-1], *plane[:-1]):
            greet(at(*to, 1))
        for to in plane:
            greet(at(*to, 0))

    @pl.when(~hub)
    def _():
        for to in near:
            greet(at(*to))
        greet(at(0, 0, 0, 1))

    loads[0].wait()
    for load in loads[1:]:
        load.start()
    total = jnp.zeros((16, LANES), jnp.float32)
    for c in range(0, width, LANES):
        part = g_in[:, c : c + LANES].astype(jnp.float32)
        total = total + part * part
    total = jnp.sum(total, axis=0, keepdims=True)

    own_buf[0] = total

    @pl.when(hub)
    def _():
        plane_buf[0] = total
        pl.semaphore_wait(barrier, len(plane) + len(line) - 1)

    @pl.when(~hub)
    def _():
        pl.semaphore_wait(barrier, len(plane) + len(near))

    def message(stage, src, dst, peer):
        return pltpu.make_async_remote_copy(
            src_ref=src,
            dst_ref=dst,
            send_sem=sum_send.at[stage],
            recv_sem=sum_recv.at[stage],
            device_id=peer,
            device_id_type=MESH,
        )

    def part_to(to):
        place = (to[0] * NY + to[2]) * 2 + 1 - core
        return message(0, own_buf.at[0], plane_buf.at[place], at(*to, 1))

    def several(stage, count):
        those = plane_buf.at[pl.ds(0, count)]
        return message(stage, those, those, at(1, 0))

    for to in plane[:-1]:
        part_to(to).start()

    @pl.when(~hub)
    def _():
        part_to(plane[-1]).start()

    @pl.when(hub)
    def _():
        several(0, 2 * len(plane) - 1).wait_recv()
        z_buf[0] = jnp.sum(plane_buf[...], axis=0)
        for to in line[:-1]:
            message(1, z_buf.at[0], z_buf.at[to[1]], at(*to, 1)).start()
        several(1, len(line) - 1).wait_recv()
        all_buf[0] = jnp.sum(z_buf[...], axis=0)
        message(1, all_buf.at[0], all_buf.at[0], at(0, 0, 0, 0)).start()

    @pl.when(~hub)
    def _():
        several(1, 1).wait_recv()

    total = all_buf[0]

    norm_total = jnp.sum(total, axis=1, keepdims=True)
    scale = jnp.minimum(1.0, 1.0 / jnp.sqrt(norm_total / entries + 1e-06))
    for load in loads[1:]:
        load.wait()

    pieces = pieces_of(width)
    sends = trees_of(pieces)
    plan = plan_of(pieces, sends)
    waits = waits_of(pieces, sends, plan)
    groups = [group for those in waits for group in those]
    slot = {place: i for i, group in enumerate(groups) for place in group}

    def view(place):
        v, ox, oz = place
        row, column, columns, *_ = pieces[v]
        source = (x - ox + NX) % NX * NZ + (z - oz + NZ) % NZ
        start = pl.multiple_of(source * 16 + row, 8)
        return rep.at[pl.ds(start, ROWS), pl.ds(column, columns)]

    def copy_of(ref, index, peer):
        return pltpu.make_async_remote_copy(
            src_ref=ref,
            dst_ref=ref,
            send_sem=send_sem.at[0],
            recv_sem=recv_sem.at[index],
            device_id=peer,
            device_id_type=MESH,
        )

    def run(step):
        for group in waits[step]:
            _, column, columns, *_ = pieces[group[0][0]]
            taken = rep.at[pl.ds(0, len(group) * ROWS), pl.ds(column, columns)]
            copy_of(taken, slot[group[0]], at(1, 0)).wait_recv()
        for send in plan[step][1] if step < len(plan) else ():
            axis, way, there = send
            peer = at(way, 0) if axis == "x" else at(0, way)
            copy_of(view(source_of(send)), slot[there], peer).start()

    correct_one = 1.0 - 0.9**10
    correct_two = 1.0 - 0.95**10
    mine = pl.multiple_of(shard * 16, 16)
    chunk = 8 * LANES
    for v, (row, column, columns, *_) in enumerate(pieces):
        rows = slice(row, row + ROWS)
        for c in range(column, column + columns, chunk):
            cols = slice(c, min(c + chunk, column + columns))
            clipped = scale * g_in[rows, cols].astype(jnp.float32)
            params = p_in[rows, cols]
            new_first = 0.9 * m_in[rows, cols] + 0.1 * clipped
            new_second = 0.95 * v_in[rows, cols] + 0.05 * clipped * clipped
            stepped = (new_first / correct_one) / (
                jnp.sqrt(new_second / correct_two) + 1e-08
            )
            new_params = params - 0.1 * (stepped + 0.1 * params)
            p_out[rows, cols] = new_params
            m_out[rows, cols] = new_first
            v_out[rows, cols] = new_second
            rep[pl.ds(mine + row, ROWS), cols] = new_params.astype(jnp.bfloat16)
        run(v)

    for i in range(len(pieces), len(plan) + 1):
        run(i)
    sent = rep.at[pl.ds(0, rep.shape[0] - 16)]
    copy_of(sent, 0, at(1, 0)).wait_send()
    @pl.when(hub)
    def _():
        several(0, len(plane) - 1).wait_send()
        several(1, len(line)).wait_send()

    @pl.when(~hub)
    def _():
        several(0, len(plane)).wait_send()


def store_kernel(rep, p_new, m_new, v_new, p_out, m_out, v_out, rep_out, sem):
    parts = 8
    rows = rep.shape[0] // parts
    copies = [
        (rep.at[pl.ds(i * rows, rows)], rep_out.at[pl.ds(i * rows, rows)])
        for i in range(parts)
    ]
    copies += [(p_new, p_out), (m_new, m_out), (v_new, v_out)]
    started = [
        pltpu.make_async_copy(src, dst, sem.at[i]) for i, (src, dst) in enumerate(copies)
    ]
    for copy in started:
        copy.start()
    for copy in started:
        copy.wait()


def on_device(params, gradient, first_moment, second_moment):
    rows, width = params.shape
    entries = rows * width * lax.axis_size("group") * lax.axis_size("shard")
    whole = (rows * lax.axis_size("shard"), width)
    f32, bf16 = jnp.float32, jnp.bfloat16
    pieces = pieces_of(width)
    sends = trees_of(pieces)
    waits = waits_of(pieces, sends, plan_of(pieces, sends))
    messages = sum(len(groups) for groups in waits)
    hbm = pl.BlockSpec(memory_space=pltpu.HBM)
    vmem = pl.BlockSpec(memory_space=pltpu.VMEM)
    rep, p_new, m_new, v_new = pl.pallas_call(
        functools.partial(step_kernel, entries),
        out_shape=(
            pltpu.VMEM(whole, bf16),
            pltpu.VMEM((rows, width), f32),
            pltpu.VMEM((rows, width), f32),
            pltpu.VMEM((rows, width), f32),
        ),
        in_specs=[hbm] * 4,
        out_specs=[vmem] * 4,
        scratch_shapes=[
            pltpu.VMEM((rows, width), f32),
            pltpu.VMEM((rows, width), bf16),
            pltpu.VMEM((rows, width), f32),
            pltpu.VMEM((rows, width), f32),
            pltpu.VMEM((1, 1, LANES), f32),
            pltpu.VMEM((NX * NY * 2, 1, LANES), f32),
            pltpu.VMEM((NZ, 1, LANES), f32),
            pltpu.VMEM((1, 1, LANES), f32),
            pltpu.SemaphoreType.DMA((4,)),
            pltpu.SemaphoreType.DMA((2,)),
            pltpu.SemaphoreType.DMA((2,)),
            pltpu.SemaphoreType.DMA((1,)),
            pltpu.SemaphoreType.DMA((messages,)),
        ],
        compiler_params=pltpu.CompilerParams(
            collective_id=0, has_side_effects=True, vmem_limit_bytes=58_200_000
        ),
        name="step",
    )(params, gradient, first_moment, second_moment)
    return pl.pallas_call(
        store_kernel,
        out_shape=(
            jax.ShapeDtypeStruct((rows, width), f32),
            jax.ShapeDtypeStruct((rows, width), f32),
            jax.ShapeDtypeStruct((rows, width), f32),
            jax.ShapeDtypeStruct(whole, bf16),
        ),
        in_specs=[vmem] * 4,
        out_specs=[hbm] * 4,
        scratch_shapes=[pltpu.SemaphoreType.DMA((11,))],
        compiler_params=pltpu.CompilerParams(vmem_limit_bytes=24 * 2**20),
        name="store",
    )(rep, p_new, m_new, v_new)


def solution(mesh):
    rows = P(("group", "shard"), None)
    return jax.shard_map(
        on_device,
        mesh=mesh,
        in_specs=(rows,) * 4,
        out_specs=(rows, rows, rows, P("group", None)),
        check_vma=False,
    )
```

```python
import functools
import heapq
import itertools

import jax
import jax.numpy as jnp
from jax import lax
from jax.experimental import pallas as pl
from jax.experimental.pallas import tpu as pltpu
from jax.sharding import PartitionSpec as P

MESH = pl.DeviceIdType.MESH
NY, NX, NZ = 4, 4, 8
LANES = 128
ROWS = 8


def pieces_of(width):
    cut = (width // LANES * 23 // 56) * LANES
    return (
        (0, cut, width - cut, False, 1, 1),
        (8, cut, width - cut, False, -1, -1),
        (0, 0, cut, True, 1, 1),
        (8, 0, cut, True, -1, -1),
    )


def trees_of(pieces):
    sends = {}
    for v, (_, _, _, x_first, sx, sz) in enumerate(pieces):
        reach = {
            "x": {sx: NX // 2, -sx: NX // 2 - 1},
            "z": {sz: NZ // 2, -sz: NZ // 2 - 1},
        }
        first, second = ("x", "z") if x_first else ("z", "x")

        def add(axis, step, a, b, a2, b2):
            here = (a, b) if x_first else (b, a)
            there = (a2, b2) if x_first else (b2, a2)
            sends.setdefault((v, *here), []).append((axis, step, (v, *there)))

        for a in range(-reach[first][-1], reach[first][1] + 1):
            for step in (1, -1):
                if a * step >= 0 and abs(a) < reach[first][step]:
                    add(first, step, a, 0, a + step, 0)
            for step in (1, -1):
                for b in range(reach[second][step]):
                    add(second, step, a, b * step, a, (b + 1) * step)
    return sends


def plan_of(pieces, sends, rate=46.6e3, latency=2.4, ahead=2.0):
    @functools.cache
    def depth(place):
        return max((1 + depth(there) for *_, there in sends.get(place, ())), default=0)

    @functools.cache
    def size(place):
        return 1 + sum(size(there) for *_, there in sends.get(place, ()))

    queues = {link: [] for link in itertools.product("xz", (1, -1))}
    free = dict.fromkeys(queues, 0.0)
    count = itertools.count()
    events = [(0.15 * v, next(count), (v, 0, 0)) for v in range(len(pieces))]
    steps, held, turns = [], {}, []
    while events:
        now = events[0][0]
        while events and events[0][0] <= now + 1e-9:
            _, _, place = heapq.heappop(events)
            if place is not None:
                for axis, step, there in sends.get(place, ()):
                    heapq.heappush(
                        queues[axis, step], (-depth(there), -size(there), next(count), there)
                    )
                    held[there] = len(steps)
                steps.append((now, place, []))
        for link, queue in queues.items():
            if queue and free[link] <= now + 1e-9:
                *_, there = heapq.heappop(queue)
                free[link] = now + pieces[there[0]][2] * ROWS * 2 / rate
                heapq.heappush(events, (free[link], next(count), None))
                heapq.heappush(events, (free[link] + latency, next(count), there))
                turns.append((now, link, there))
    last = dict.fromkeys(queues, 0)
    for turn, link, there in turns:
        i = held[there]
        while i + 1 < len(steps) and steps[i + 1][0] <= turn - ahead:
            i += 1
        last[link] = max(i, last[link])
        steps[last[link]][2].append((*link, there))
    return [(place, starts) for _, place, starts in steps]


def source_of(send):
    axis, step, (v, ox, oz) = send
    return (v, ox - step, oz) if axis == "x" else (v, ox, oz - step)


def waits_of(pieces, sends, plan):
    there_by = {place: i for i, (place, _) in enumerate(plan)}
    needed = {}
    for i, (_, starts) in enumerate(plan):
        for send in starts:
            needed.setdefault(source_of(send), i)
    waits = [[] for _ in range(len(plan) + 1)]
    for size in sorted({piece[1:3] for piece in pieces}):
        left = sorted(
            (needed.get(place, len(plan)), i, place)
            for place, i in there_by.items()
            if i >= len(pieces) and pieces[place[0]][1:3] == size
        )
        while left:
            at = left[0][0]
            waits[at].append([place for _, i, place in left if i <= at])
            left = [entry for entry in left if entry[1] > at]
    return waits


def far_first(offsets):
    def chips(to):
        sizes = (NX, NZ, NY)
        return sum(min(step, size - step) for step, size in zip(to, sizes))

    return sorted(offsets, key=chips, reverse=True)


def step_kernel(
    entries,
    p_hbm,
    g_hbm,
    m_hbm,
    v_hbm,
    rep,
    p_out,
    m_out,
    v_out,
    p_in,
    g_in,
    m_in,
    v_in,
    own_buf,
    plane_buf,
    z_buf,
    all_buf,
    load_sem,
    sum_send,
    sum_recv,
    send_sem,
    recv_sem,
):
    width = g_hbm.shape[1]
    group = lax.axis_index("group")
    shard = lax.axis_index("shard")
    x, z = shard // NZ, shard % NZ

    y, core = group // 2, group % 2
    hub = core == 1

    def at(dx, dz, dy=0, to_core=core):
        to = (x + dx + NX) % NX * NZ + (z + dz + NZ) % NZ
        return ((y + dy + NY) % NY * 2 + to_core, to)

    loads = [
        pltpu.make_async_copy(src, dst, load_sem.at[i])
        for i, (src, dst) in enumerate(
            ((g_hbm, g_in), (p_hbm, p_in), (m_hbm, m_in), (v_hbm, v_in))
        )
    ]
    loads[0].start()

    plane = far_first((dx, 0, dy) for dx in range(NX) for dy in range(NY))
    line = far_first((0, dz, 0) for dz in range(NZ))
    near = ((1, 0), (-1, 0), (0, 1), (0, -1))
    barrier = pltpu.get_barrier_semaphore()

    def greet(peer):
        pl.semaphore_signal(barrier, inc=1, device_id=peer, device_id_type=MESH)

    @pl.when(hub)
    def _():
        for to in (*line[:-1], *plane[:-1]):
            greet(at(*to, 1))
        for to in plane:
            greet(at(*to, 0))

    @pl.when(~hub)
    def _():
        for to in near:
            greet(at(*to))
        greet(at(0, 0, 0, 1))

    loads[0].wait()
    for load in loads[1:]:
        load.start()
    total = jnp.zeros((16, LANES), jnp.float32)
    for c in range(0, width, LANES):
        part = g_in[:, c : c + LANES].astype(jnp.float32)
        total = total + part * part
    total = jnp.sum(total, axis=0, keepdims=True)

    own_buf[0] = total

    @pl.when(hub)
    def _():
        plane_buf[0] = total
        pl.semaphore_wait(barrier, len(plane) + len(line) - 1)

    @pl.when(~hub)
    def _():
        pl.semaphore_wait(barrier, len(plane) + len(near))

    def message(stage, src, dst, peer):
        return pltpu.make_async_remote_copy(
            src_ref=src,
            dst_ref=dst,
            send_sem=sum_send.at[stage],
            recv_sem=sum_recv.at[stage],
            device_id=peer,
            device_id_type=MESH,
        )

    def part_to(to):
        place = (to[0] * NY + to[2]) * 2 + 1 - core
        return message(0, own_buf.at[0], plane_buf.at[place], at(*to, 1))

    def several(stage, count):
        those = plane_buf.at[pl.ds(0, count)]
        return message(stage, those, those, at(1, 0))

    for to in plane[:-1]:
        part_to(to).start()

    @pl.when(~hub)
    def _():
        part_to(plane[-1]).start()

    @pl.when(hub)
    def _():
        several(0, 2 * len(plane) - 1).wait_recv()
        z_buf[0] = jnp.sum(plane_buf[...], axis=0)
        for to in line[:-1]:
            message(1, z_buf.at[0], z_buf.at[to[1]], at(*to, 1)).start()
        several(1, len(line) - 1).wait_recv()
        all_buf[0] = jnp.sum(z_buf[...], axis=0)
        message(1, all_buf.at[0], all_buf.at[0], at(0, 0, 0, 0)).start()

    @pl.when(~hub)
    def _():
        several(1, 1).wait_recv()

    total = all_buf[0]

    norm_total = jnp.sum(total, axis=1, keepdims=True)
    scale = jnp.minimum(1.0, 1.0 / jnp.sqrt(norm_total / entries + 1e-06))
    for load in loads[1:]:
        load.wait()

    pieces = pieces_of(width)
    sends = trees_of(pieces)
    plan = plan_of(pieces, sends)
    waits = waits_of(pieces, sends, plan)
    groups = [group for those in waits for group in those]
    slot = {place: i for i, group in enumerate(groups) for place in group}

    def view(place):
        v, ox, oz = place
        row, column, columns, *_ = pieces[v]
        source = (x - ox + NX) % NX * NZ + (z - oz + NZ) % NZ
        start = pl.multiple_of(source * 16 + row, 8)
        return rep.at[pl.ds(start, ROWS), pl.ds(column, columns)]

    def copy_of(ref, index, peer):
        return pltpu.make_async_remote_copy(
            src_ref=ref,
            dst_ref=ref,
            send_sem=send_sem.at[0],
            recv_sem=recv_sem.at[index],
            device_id=peer,
            device_id_type=MESH,
        )

    def run(step):
        for group in waits[step]:
            _, column, columns, *_ = pieces[group[0][0]]
            taken = rep.at[pl.ds(0, len(group) * ROWS), pl.ds(column, columns)]
            copy_of(taken, slot[group[0]], at(1, 0)).wait_recv()
        for send in plan[step][1] if step < len(plan) else ():
            axis, way, there = send
            peer = at(way, 0) if axis == "x" else at(0, way)
            copy_of(view(source_of(send)), slot[there], peer).start()

    correct_one = 1.0 - 0.9**10
    correct_two = 1.0 - 0.95**10
    mine = pl.multiple_of(shard * 16, 16)
    chunk = 8 * LANES
    for v, (row, column, columns, *_) in enumerate(pieces):
        rows = slice(row, row + ROWS)
        for c in range(column, column + columns, chunk):
            cols = slice(c, min(c + chunk, column + columns))
            clipped = scale * g_in[rows, cols].astype(jnp.float32)
            params = p_in[rows, cols]
            new_first = 0.9 * m_in[rows, cols] + 0.1 * clipped
            new_second = 0.95 * v_in[rows, cols] + 0.05 * clipped * clipped
            stepped = (new_first / correct_one) / (
                jnp.sqrt(new_second / correct_two) + 1e-08
            )
            new_params = params - 0.1 * (stepped + 0.1 * params)
            p_out[rows, cols] = new_params
            m_out[rows, cols] = new_first
            v_out[rows, cols] = new_second
            rep[pl.ds(mine + row, ROWS), cols] = new_params.astype(jnp.bfloat16)
        run(v)

    for i in range(len(pieces), len(plan) + 1):
        run(i)
    sent = rep.at[pl.ds(0, rep.shape[0] - 16)]
    copy_of(sent, 0, at(1, 0)).wait_send()
    @pl.when(hub)
    def _():
        several(0, len(plane) - 1).wait_send()
        several(1, len(line)).wait_send()

    @pl.when(~hub)
    def _():
        several(0, len(plane)).wait_send()


def store_kernel(rep, p_new, m_new, v_new, p_out, m_out, v_out, rep_out, sem):
    parts = 4
    rows = rep.shape[0] // parts
    copies = [
        (rep.at[pl.ds(i * rows, rows)], rep_out.at[pl.ds(i * rows, rows)])
        for i in range(parts)
    ]
    copies += [(p_new, p_out), (m_new, m_out), (v_new, v_out)]
    for i, (src, dst) in enumerate(copies):
        pltpu.make_async_copy(src, dst, sem.at[max(i - parts + 1, 0)]).start()
    whole = [(rep, rep_out), *copies[parts:]]
    for i, (src, dst) in enumerate(whole):
        pltpu.make_async_copy(src, dst, sem.at[i]).wait()


def on_device(params, gradient, first_moment, second_moment):
    rows, width = params.shape
    entries = rows * width * lax.axis_size("group") * lax.axis_size("shard")
    whole = (rows * lax.axis_size("shard"), width)
    f32, bf16 = jnp.float32, jnp.bfloat16
    pieces = pieces_of(width)
    sends = trees_of(pieces)
    waits = waits_of(pieces, sends, plan_of(pieces, sends))
    messages = sum(len(groups) for groups in waits)
    hbm = pl.BlockSpec(memory_space=pltpu.HBM)
    vmem = pl.BlockSpec(memory_space=pltpu.VMEM)
    rep, p_new, m_new, v_new = pl.pallas_call(
        functools.partial(step_kernel, entries),
        out_shape=(
            pltpu.VMEM(whole, bf16),
            pltpu.VMEM((rows, width), f32),
            pltpu.VMEM((rows, width), f32),
            pltpu.VMEM((rows, width), f32),
        ),
        in_specs=[hbm] * 4,
        out_specs=[vmem] * 4,
        scratch_shapes=[
            pltpu.VMEM((rows, width), f32),
            pltpu.VMEM((rows, width), bf16),
            pltpu.VMEM((rows, width), f32),
            pltpu.VMEM((rows, width), f32),
            pltpu.VMEM((1, 1, LANES), f32),
            pltpu.VMEM((NX * NY * 2, 1, LANES), f32),
            pltpu.VMEM((NZ, 1, LANES), f32),
            pltpu.VMEM((1, 1, LANES), f32),
            pltpu.SemaphoreType.DMA((4,)),
            pltpu.SemaphoreType.DMA((2,)),
            pltpu.SemaphoreType.DMA((2,)),
            pltpu.SemaphoreType.DMA((1,)),
            pltpu.SemaphoreType.DMA((messages,)),
        ],
        compiler_params=pltpu.CompilerParams(
            collective_id=0, has_side_effects=True, vmem_limit_bytes=58_200_000
        ),
        name="step",
    )(params, gradient, first_moment, second_moment)
    return pl.pallas_call(
        store_kernel,
        out_shape=(
            jax.ShapeDtypeStruct((rows, width), f32),
            jax.ShapeDtypeStruct((rows, width), f32),
            jax.ShapeDtypeStruct((rows, width), f32),
            jax.ShapeDtypeStruct(whole, bf16),
        ),
        in_specs=[vmem] * 4,
        out_specs=[hbm] * 4,
        scratch_shapes=[pltpu.SemaphoreType.DMA((4,))],
        compiler_params=pltpu.CompilerParams(vmem_limit_bytes=24 * 2**20),
        name="store",
    )(rep, p_new, m_new, v_new)


def solution(mesh):
    rows = P(("group", "shard"), None)
    return jax.shard_map(
        on_device,
        mesh=mesh,
        in_specs=(rows,) * 4,
        out_specs=(rows, rows, rows, P("group", None)),
        check_vma=False,
    )
```

```python
import functools
import heapq
import itertools

import jax
import jax.numpy as jnp
from jax import lax
from jax.experimental import pallas as pl
from jax.experimental.pallas import tpu as pltpu
from jax.sharding import PartitionSpec as P

MESH = pl.DeviceIdType.MESH
NY, NX, NZ = 4, 4, 8
LANES = 128
ROWS = 8


def pieces_of(width):
    upper, lower = (width // LANES * part // 56 * LANES for part in (23, 22))
    return (
        (0, upper, width - upper, False, 1, 1),
        (8, lower, width - lower, False, -1, -1),
        (0, 0, upper, True, 1, 1),
        (8, 0, lower, True, -1, -1),
    )


def trees_of(pieces):
    sends = {}
    for v, (_, _, _, x_first, sx, sz) in enumerate(pieces):
        reach = {
            "x": {sx: NX // 2, -sx: NX // 2 - 1},
            "z": {sz: NZ // 2, -sz: NZ // 2 - 1},
        }
        first, second = ("x", "z") if x_first else ("z", "x")

        def add(axis, step, a, b, a2, b2):
            here = (a, b) if x_first else (b, a)
            there = (a2, b2) if x_first else (b2, a2)
            sends.setdefault((v, *here), []).append((axis, step, (v, *there)))

        for a in range(-reach[first][-1], reach[first][1] + 1):
            for step in (1, -1):
                if a * step >= 0 and abs(a) < reach[first][step]:
                    add(first, step, a, 0, a + step, 0)
            for step in (1, -1):
                for b in range(reach[second][step]):
                    add(second, step, a, b * step, a, (b + 1) * step)
    return sends


def plan_of(pieces, sends, rate=46.6e3, latency=2.4, ahead=2.0):
    @functools.cache
    def depth(place):
        return max((1 + depth(there) for *_, there in sends.get(place, ())), default=0)

    @functools.cache
    def size(place):
        return 1 + sum(size(there) for *_, there in sends.get(place, ()))

    queues = {link: [] for link in itertools.product("xz", (1, -1))}
    free = dict.fromkeys(queues, 0.0)
    count = itertools.count()
    events = [(0.15 * v, next(count), (v, 0, 0)) for v in range(len(pieces))]
    steps, held, turns = [], {}, []
    while events:
        now = events[0][0]
        while events and events[0][0] <= now + 1e-9:
            _, _, place = heapq.heappop(events)
            if place is not None:
                for axis, step, there in sends.get(place, ()):
                    heapq.heappush(
                        queues[axis, step], (-depth(there), -size(there), next(count), there)
                    )
                    held[there] = len(steps)
                steps.append((now, place, []))
        for link, queue in queues.items():
            if queue and free[link] <= now + 1e-9:
                *_, there = heapq.heappop(queue)
                free[link] = now + pieces[there[0]][2] * ROWS * 2 / rate
                heapq.heappush(events, (free[link], next(count), None))
                heapq.heappush(events, (free[link] + latency, next(count), there))
                turns.append((now, link, there))
    last = dict.fromkeys(queues, 0)
    for turn, link, there in turns:
        i = held[there]
        while i + 1 < len(steps) and steps[i + 1][0] <= turn - ahead:
            i += 1
        last[link] = max(i, last[link])
        steps[last[link]][2].append((*link, there))
    return [(place, starts) for _, place, starts in steps]


def source_of(send):
    axis, step, (v, ox, oz) = send
    return (v, ox - step, oz) if axis == "x" else (v, ox, oz - step)


def waits_of(pieces, sends, plan):
    there_by = {place: i for i, (place, _) in enumerate(plan)}
    needed = {}
    for i, (_, starts) in enumerate(plan):
        for send in starts:
            needed.setdefault(source_of(send), i)
    waits = [[] for _ in range(len(plan) + 1)]
    for size in sorted({piece[1:3] for piece in pieces}):
        left = sorted(
            (needed.get(place, len(plan)), i, place)
            for place, i in there_by.items()
            if i >= len(pieces) and pieces[place[0]][1:3] == size
        )
        while left:
            at = left[0][0]
            waits[at].append([place for _, i, place in left if i <= at])
            left = [entry for entry in left if entry[1] > at]
    return waits


def far_first(offsets):
    def chips(to):
        sizes = (NX, NZ, NY)
        return sum(min(step, size - step) for step, size in zip(to, sizes))

    return sorted(offsets, key=chips, reverse=True)


def step_kernel(
    entries,
    p_hbm,
    g_hbm,
    m_hbm,
    v_hbm,
    rep,
    p_out,
    m_out,
    v_out,
    p_in,
    g_in,
    m_in,
    v_in,
    own_buf,
    plane_buf,
    z_buf,
    all_buf,
    load_sem,
    sum_send,
    sum_recv,
    send_sem,
    recv_sem,
):
    width = g_hbm.shape[1]
    group = lax.axis_index("group")
    shard = lax.axis_index("shard")
    x, z = shard // NZ, shard % NZ

    y, core = group // 2, group % 2
    hub = core == 1

    turn = 1 - 2 * core

    def at(dx, dz, dy=0, to_core=core):
        to = (x + dx + NX) % NX * NZ + (z + dz + NZ) % NZ
        return ((y + dy + NY) % NY * 2 + to_core, to)

    loads = [
        pltpu.make_async_copy(src, dst, load_sem.at[i])
        for i, (src, dst) in enumerate(
            ((g_hbm, g_in), (p_hbm, p_in), (m_hbm, m_in), (v_hbm, v_in))
        )
    ]
    loads[0].start()

    plane = far_first((dx, 0, dy) for dx in range(NX) for dy in range(NY))
    line = far_first((0, dz, 0) for dz in range(NZ))
    near = ((1, 0), (-1, 0), (0, 1), (0, -1))
    barrier = pltpu.get_barrier_semaphore()

    def greet(peer):
        pl.semaphore_signal(barrier, inc=1, device_id=peer, device_id_type=MESH)

    @pl.when(hub)
    def _():
        for to in (*line[:-1], *plane[:-1]):
            greet(at(*to, 1))
        for to in plane:
            greet(at(*to, 0))

    @pl.when(~hub)
    def _():
        for to in near:
            greet(at(*to))
        greet(at(0, 0, 0, 1))

    loads[0].wait()
    for load in loads[1:]:
        load.start()
    total = jnp.zeros((16, LANES), jnp.float32)
    for c in range(0, width, LANES):
        part = g_in[:, c : c + LANES].astype(jnp.float32)
        total = total + part * part
    total = jnp.sum(total, axis=0, keepdims=True)

    own_buf[0] = total

    @pl.when(hub)
    def _():
        plane_buf[0] = total
        pl.semaphore_wait(barrier, len(plane) + len(line) - 1)

    @pl.when(~hub)
    def _():
        pl.semaphore_wait(barrier, len(plane) + len(near))

    def message(stage, src, dst, peer):
        return pltpu.make_async_remote_copy(
            src_ref=src,
            dst_ref=dst,
            send_sem=sum_send.at[stage],
            recv_sem=sum_recv.at[stage],
            device_id=peer,
            device_id_type=MESH,
        )

    def part_to(to):
        place = (to[0] * NY + to[2]) * 2 + 1 - core
        return message(0, own_buf.at[0], plane_buf.at[place], at(*to, 1))

    def several(stage, count):
        those = plane_buf.at[pl.ds(0, count)]
        return message(stage, those, those, at(1, 0))

    for to in plane[:-1]:
        part_to(to).start()

    @pl.when(~hub)
    def _():
        part_to(plane[-1]).start()

    @pl.when(hub)
    def _():
        several(0, 2 * len(plane) - 1).wait_recv()
        z_buf[0] = jnp.sum(plane_buf[...], axis=0)
        for to in line[:-1]:
            message(1, z_buf.at[0], z_buf.at[to[1]], at(*to, 1)).start()
        several(1, len(line) - 1).wait_recv()
        all_buf[0] = jnp.sum(z_buf[...], axis=0)
        message(1, all_buf.at[0], all_buf.at[0], at(0, 0, 0, 0)).start()

    @pl.when(~hub)
    def _():
        several(1, 1).wait_recv()

    total = all_buf[0]

    norm_total = jnp.sum(total, axis=1, keepdims=True)
    scale = jnp.minimum(1.0, 1.0 / jnp.sqrt(norm_total / entries + 1e-06))
    for load in loads[1:]:
        load.wait()

    pieces = pieces_of(width)
    sends = trees_of(pieces)
    plan = plan_of(pieces, sends)
    waits = waits_of(pieces, sends, plan)
    groups = [group for those in waits for group in those]
    slot = {place: i for i, group in enumerate(groups) for place in group}

    def view(place):
        v, ox, oz = place
        row, column, columns, *_ = pieces[v]
        source = (x - turn * ox + NX) % NX * NZ + (z - oz + NZ) % NZ
        start = pl.multiple_of(source * 16 + row, 8)
        return rep.at[pl.ds(start, ROWS), pl.ds(column, columns)]

    def copy_of(ref, index, peer):
        return pltpu.make_async_remote_copy(
            src_ref=ref,
            dst_ref=ref,
            send_sem=send_sem.at[0],
            recv_sem=recv_sem.at[index],
            device_id=peer,
            device_id_type=MESH,
        )

    def run(step):
        for group in waits[step]:
            _, column, columns, *_ = pieces[group[0][0]]
            taken = rep.at[pl.ds(0, len(group) * ROWS), pl.ds(column, columns)]
            copy_of(taken, slot[group[0]], at(1, 0)).wait_recv()
        for send in plan[step][1] if step < len(plan) else ():
            axis, way, there = send
            peer = at(turn * way, 0) if axis == "x" else at(0, way)
            copy_of(view(source_of(send)), slot[there], peer).start()

    correct_one = 1.0 - 0.9**10
    correct_two = 1.0 - 0.95**10
    mine = pl.multiple_of(shard * 16, 16)
    chunk = 8 * LANES
    for v, (row, column, columns, *_) in enumerate(pieces):
        rows = slice(row, row + ROWS)
        for c in range(column, column + columns, chunk):
            cols = slice(c, min(c + chunk, column + columns))
            clipped = scale * g_in[rows, cols].astype(jnp.float32)
            params = p_in[rows, cols]
            new_first = 0.9 * m_in[rows, cols] + 0.1 * clipped
            new_second = 0.95 * v_in[rows, cols] + 0.05 * clipped * clipped
            stepped = (new_first / correct_one) / (
                jnp.sqrt(new_second / correct_two) + 1e-08
            )
            new_params = params - 0.1 * (stepped + 0.1 * params)
            p_out[rows, cols] = new_params
            m_out[rows, cols] = new_first
            v_out[rows, cols] = new_second
            rep[pl.ds(mine + row, ROWS), cols] = new_params.astype(jnp.bfloat16)
        run(v)

    for i in range(len(pieces), len(plan) + 1):
        run(i)
    sent = rep.at[pl.ds(0, rep.shape[0] - 16)]
    copy_of(sent, 0, at(1, 0)).wait_send()
    @pl.when(hub)
    def _():
        several(0, len(plane) - 1).wait_send()
        several(1, len(line)).wait_send()

    @pl.when(~hub)
    def _():
        several(0, len(plane)).wait_send()


def store_kernel(rep, p_new, m_new, v_new, p_out, m_out, v_out, rep_out, sem):
    parts = 4
    rows = rep.shape[0] // parts
    copies = [
        (rep.at[pl.ds(i * rows, rows)], rep_out.at[pl.ds(i * rows, rows)])
        for i in range(parts)
    ]
    copies += [(p_new, p_out), (m_new, m_out), (v_new, v_out)]
    for i, (src, dst) in enumerate(copies):
        pltpu.make_async_copy(src, dst, sem.at[max(i - parts + 1, 0)]).start()
    whole = [(rep, rep_out), *copies[parts:]]
    for i, (src, dst) in enumerate(whole):
        pltpu.make_async_copy(src, dst, sem.at[i]).wait()


def on_device(params, gradient, first_moment, second_moment):
    rows, width = params.shape
    entries = rows * width * lax.axis_size("group") * lax.axis_size("shard")
    whole = (rows * lax.axis_size("shard"), width)
    f32, bf16 = jnp.float32, jnp.bfloat16
    pieces = pieces_of(width)
    sends = trees_of(pieces)
    waits = waits_of(pieces, sends, plan_of(pieces, sends))
    messages = sum(len(groups) for groups in waits)
    hbm = pl.BlockSpec(memory_space=pltpu.HBM)
    vmem = pl.BlockSpec(memory_space=pltpu.VMEM)
    rep, p_new, m_new, v_new = pl.pallas_call(
        functools.partial(step_kernel, entries),
        out_shape=(
            pltpu.VMEM(whole, bf16),
            pltpu.VMEM((rows, width), f32),
            pltpu.VMEM((rows, width), f32),
            pltpu.VMEM((rows, width), f32),
        ),
        in_specs=[hbm] * 4,
        out_specs=[vmem] * 4,
        scratch_shapes=[
            pltpu.VMEM((rows, width), f32),
            pltpu.VMEM((rows, width), bf16),
            pltpu.VMEM((rows, width), f32),
            pltpu.VMEM((rows, width), f32),
            pltpu.VMEM((1, 1, LANES), f32),
            pltpu.VMEM((NX * NY * 2, 1, LANES), f32),
            pltpu.VMEM((NZ, 1, LANES), f32),
            pltpu.VMEM((1, 1, LANES), f32),
            pltpu.SemaphoreType.DMA((4,)),
            pltpu.SemaphoreType.DMA((2,)),
            pltpu.SemaphoreType.DMA((2,)),
            pltpu.SemaphoreType.DMA((1,)),
            pltpu.SemaphoreType.DMA((messages,)),
        ],
        compiler_params=pltpu.CompilerParams(
            collective_id=0, has_side_effects=True, vmem_limit_bytes=58_200_000
        ),
        name="step",
    )(params, gradient, first_moment, second_moment)
    return pl.pallas_call(
        store_kernel,
        out_shape=(
            jax.ShapeDtypeStruct((rows, width), f32),
            jax.ShapeDtypeStruct((rows, width), f32),
            jax.ShapeDtypeStruct((rows, width), f32),
            jax.ShapeDtypeStruct(whole, bf16),
        ),
        in_specs=[vmem] * 4,
        out_specs=[hbm] * 4,
        scratch_shapes=[pltpu.SemaphoreType.DMA((4,))],
        compiler_params=pltpu.CompilerParams(vmem_limit_bytes=24 * 2**20),
        name="store",
    )(rep, p_new, m_new, v_new)


def solution(mesh):
    rows = P(("group", "shard"), None)
    return jax.shard_map(
        on_device,
        mesh=mesh,
        in_specs=(rows,) * 4,
        out_specs=(rows, rows, rows, P("group", None)),
        check_vma=False,
    )
```
